32 devices in a mesh: groups: 2 (over x), seq: 8 (over z, y), head: 2 (over core).
Axes of the slice: x: 2, y: 2, z: 4, core: 2. Of those that a mesh axis runs over, the one named last changes fastest.
Arguments:
- q_latent: bfloat16 [16, 64, 512], P(('groups', 'seq'), 'head'), parts along dimension 0, may hold values from -7.5 to 7.5
- q_rope: bfloat16 [16, 4096], P(('groups', 'seq'), 'head'), parts along dimension 0, may hold values from -7.5 to 7.5
- cache_latent: bfloat16 [768, 64, 512], P(('groups', 'seq', 'head')), parts along dimension 0, may hold values from -10 to 10
- cache_rope: bfloat16 [768, 4096], P(('groups', 'seq', 'head')), parts along dimension 0, may hold values from -6 to 6
- page_table: int32 [16, 48], P('groups'), parts along dimension 0, may hold values from 0 to 383, as said below
- lengths: int32 [16], P('groups'), parts along dimension 0, may hold values from 1 to 3072, 14745 in all
Outputs:
- attended: bfloat16 [16, 64, 512], P(('groups', 'seq'), 'head'), parts along dimension 0
The draws below stay inside these ranges and needn't reach their ends.
There are 2 independent parts, one for each index of `groups`. The reference program is written for one: setup_inputs(seed, part) draws one part's arguments, and reference() takes and returns one part's arrays. A program takes and returns all parts, laid end to end along the dimension named above; each array names one. Nothing has to cross between parts.
Inputs may be any that keep to these rules, and one draw needn't show every extreme that they name: `page_table`: device d of a group (d = seq index * 2 + head index) holds pool pages d * 24 to (d + 1) * 24 - 1. Each pool page is named exactly once. A request's logical pages k * 3 to (k + 1) * 3 - 1 lie on one device, and every device holds exactly one such run of every request. `lengths`: the newest token is counted.
All inputs are finite; a program needn't handle non-finite values.
Results may differ from the reference program's by a relative error of at most 0.0055.
Values may be sent and summed in bfloat16 or wider, within the bound.
A program may use at most 128 MiB of HBM per device.

```python
import math
import jax
import jax.numpy as jnp
import numpy as np
from jax import lax

H = 64
LAT = 512
ROPE = 64
NOPE = 128
PAGE = 64
RUN = 3
REQS = 8
DEVS = 16
POOL_DEV = 24
POOL = 384
MAXP = 48
CTX = 3072


def draw_q_latent(key, part):
    base_draw = 1.5 * jnp.clip(jax.random.normal(jax.random.fold_in(key, 5), (REQS, H, LAT), jnp.float32), -5.0, 5.0)
    return base_draw.astype(jnp.bfloat16)


def draw_cache_latent(key, part):
    base_draw = jnp.clip(jax.random.normal(jax.random.fold_in(key, 7), (POOL, PAGE, LAT), jnp.float32), -5.0, 5.0)
    return base_draw.astype(jnp.bfloat16)


def draw_page_table(key, part):
    owner_key, slot_key = jax.random.split(jax.random.fold_in(key, 11))
    owner_keys = jax.random.split(owner_key, REQS)
    run_owners = jax.vmap(lambda single: jax.random.permutation(single, DEVS))(owner_keys).astype(jnp.int32)
    slot_keys = jax.random.split(slot_key, DEVS)
    slot_perm = jax.vmap(lambda single: jax.random.permutation(single, POOL_DEV))(slot_keys).astype(jnp.int32)
    run_ids = jnp.arange(RUN, dtype=jnp.int32)
    req_ids = jnp.arange(REQS, dtype=jnp.int32)
    local_slot = slot_perm[run_owners[:, :, None], req_ids[:, None, None] * RUN + run_ids[None, None, :]]
    page_ids = run_owners[:, :, None] * POOL_DEV + local_slot
    return page_ids.reshape(REQS, MAXP).astype(jnp.int32)


def block_levels(key, extent, pieces, low, largest):
    factor_of, own = 1.0, jax.random.fold_in(key, 6)
    for dim, parts in pieces:
        draws = jnp.exp(jax.random.uniform(jax.random.fold_in(own, dim), (parts,), jnp.float32, low / len(pieces), largest / len(pieces)))
        factor_of = factor_of * jnp.repeat(draws, extent[dim] // parts).reshape([-1 if axis == dim else 1 for axis in range(len(extent))])
    return factor_of


def split_up(number_of, total, most, skew):
    portions = [(1 << 20) // math.isqrt(standing ** skew) + 1 for standing in range(2, number_of + 1)]
    rest, holding = total - most - (number_of - 1), [1] * (number_of - 1)
    while rest > 0:
        free = [i for i in range(number_of - 1) if holding[i] < most]
        pool, budget = sum([portions[i] for i in free]), rest
        for i in free:
            more = min(most - holding[i], max(1, budget * portions[i] // pool), rest)
            holding[i] = holding[i] + more
            rest = rest - more
    return np.array([most] + holding)


def uneven(key, number_of, total, limit, lean):
    if number_of == 2:
        one = jax.random.randint(key, (), max(1, total - limit), min(limit, total - 1) + 1)
        return jnp.stack([one, total - one])
    sizes = jnp.asarray(split_up(number_of, total, limit, lean), jnp.int32)
    pairs = (number_of - 1) // 2
    source_of, receiver = sizes[1:1 + 2 * pairs:2], sizes[2:2 + 2 * pairs:2]
    room = jnp.minimum(source_of - 1, limit - receiver)
    moved = jax.random.randint(jax.random.fold_in(key, 1), (pairs,), 0, 1 << 20) % (room + 1)
    sizes = sizes.at[1:1 + 2 * pairs:2].set(source_of - moved).at[2:2 + 2 * pairs:2].set(receiver + moved)
    return sizes[jax.random.permutation(jax.random.fold_in(key, 2), number_of)]


def scatter_about(own_key, extent, deviation, most, pieces=(), held_as=jnp.bfloat16):
    values = jax.random.normal(own_key, extent, jnp.float32) * deviation
    if len(pieces) > 0:
        values = block_levels(own_key, extent, pieces, -0.22, 0.18) * values
    return jnp.clip(values, min=-most, max=most).astype(held_as)


def setup_inputs(seed: int = 0, part: int = 0) -> dict:
    seeds = jax.random.split(jax.random.key(seed), 7)
    part_splits = jax.random.split(jax.random.fold_in(seeds[6], part), 7)
    q_latent = draw_q_latent(jax.random.fold_in(jax.random.fold_in(seeds[6], part), 71), part)
    q_rope = scatter_about(part_splits[1], (REQS, H * ROPE), 1.5, 7.5, ((0, 8), (1, 2)))
    cache_latent = draw_cache_latent(jax.random.fold_in(jax.random.fold_in(seeds[6], part), 71), part)
    cache_rope = scatter_about(part_splits[3], (POOL, PAGE * ROPE), 1.0, 6.0, ((0, 16),))
    page_table = draw_page_table(jax.random.fold_in(jax.random.fold_in(seeds[6], part), 71), part)
    lengths = uneven(part_splits[5], REQS, REQS * CTX * 3 // 5, CTX, 2).astype(jnp.int32)
    return dict(q_latent=q_latent, q_rope=q_rope, cache_latent=cache_latent, cache_rope=cache_rope, page_table=page_table, lengths=lengths)


MASKED_SCORE = -1e+30

def reference(q_latent, q_rope, cache_latent, cache_rope, page_table, lengths):
    score_scale = 1.0 / math.sqrt(NOPE + ROPE)
    positions = jnp.arange(MAXP * PAGE, dtype=jnp.int32)

    def attend_one(inputs_row):
        query_lat, query_rot, page_ids, seq_len = inputs_row
        key_rows = cache_latent[page_ids].reshape(MAXP * PAGE, LAT)
        rotary = cache_rope[page_ids].reshape(MAXP * PAGE, ROPE)
        scores = jnp.dot(query_lat, key_rows.T, preferred_element_type=jnp.float32)
        scores = scores + jnp.dot(query_rot.reshape(H, ROPE), rotary.T, preferred_element_type=jnp.float32)
        scores = scores * score_scale
        live_mask = positions < seq_len
        scores = jnp.where(live_mask[None, :], scores, MASKED_SCORE)
        row_max = lax.optimization_barrier(jnp.max(scores, axis=1, keepdims=True))
        exp_terms = jnp.where(live_mask[None, :], jnp.exp(scores - row_max), 0.0)
        row_total = lax.optimization_barrier(jnp.sum(exp_terms, axis=1, keepdims=True))
        weights = exp_terms.astype(jnp.bfloat16)
        summed = jnp.dot(weights, key_rows, preferred_element_type=jnp.float32)
        return (summed / row_total).astype(jnp.bfloat16)
    return lax.map(attend_one, (q_latent, q_rope, page_table, lengths))
```

```python
import functools
import math

import jax
import jax.numpy as jnp
from jax import lax
from jax.experimental import pallas as pl
from jax.experimental.pallas import tpu as pltpu
from jax.sharding import PartitionSpec as P

ROPE = 64
NOPE = 128
LANES = 128
MASKED_SCORE = -1e30


def flip(index, mask, count):
    result = index
    bit = 1
    while bit < count:
        if mask & bit:
            result = result + bit * (1 - 2 * ((index // bit) % 2))
        bit *= 2
    return result


def kernel(
    seq_count,
    run_len,
    qlat_hbm,
    qrot_hbm,
    lat_hbm,
    rot_hbm,
    table_hbm,
    len_hbm,
    out_ref,
    cache,
    rot_raw,
    rot_wide,
    rot_keys,
    qlat,
    qrot,
    qrot_rows,
    qrot_wide,
    part_send,
    part_recv,
    stat_send,
    stat_recv,
    table,
    lens,
    picks,
    local_sem,
    page_send_sem,
    page_recv_sem,
    q_send_sem,
    q_recv_sem,
    p_send_sem,
    p_recv_sem,
):
    me = lax.axis_index("seq")
    core = lax.axis_index("head")
    pool, page_len, latent = lat_hbm.shape
    heads = qlat.shape[1]
    rope = qrot.shape[2] // heads
    per_row = LANES // rope
    requests, slots = table.shape
    runs = slots // run_len
    scale = 1.0 / math.sqrt(NOPE + ROPE)

    loads = [
        pltpu.make_async_copy(qlat_hbm, qlat.at[pl.ds(0, 1)], local_sem.at[0]),
        pltpu.make_async_copy(qrot_hbm, qrot.at[0], local_sem.at[1]),
        pltpu.make_async_copy(table_hbm, table, local_sem.at[2]),
        pltpu.make_async_copy(len_hbm, lens, local_sem.at[3]),
        pltpu.make_async_copy(rot_hbm, rot_raw.at[0], local_sem.at[4]),
        pltpu.make_async_copy(lat_hbm, cache.at[0], local_sem.at[5]),
    ]
    for load in loads:
        load.start()

    barrier = pltpu.get_barrier_semaphore()
    for k in range(1, seq_count):
        pl.semaphore_signal(barrier, inc=1, device_id={"seq": flip(me, k, seq_count)})
    pl.semaphore_signal(barrier, inc=1, device_id={"head": 1 - core})

    loads[2].wait()
    loads[3].wait()
    base0 = (me * 2 + core) * pool
    base1 = (me * 2 + 1 - core) * pool

    chunk = math.gcd(runs, 16)

    def find(r, carry):
        def scan(c, found):
            run0, run1 = found
            for i in range(chunk):
                run = c * chunk + i
                first = table[r, run * run_len]
                run0 = jnp.where((first >= base0) & (first < base0 + pool), run, run0)
                run1 = jnp.where((first >= base1) & (first < base1 + pool), run, run1)
            return run0, run1

        zero = jnp.int32(0)
        if runs == chunk:
            run0, run1 = scan(0, (zero, zero))
        else:
            run0, run1 = lax.fori_loop(0, runs // chunk, scan, (zero, zero))
        for j in range(run_len):
            slot0 = table[r, run0 * run_len + j] - base0
            slot1 = table[r, run1 * run_len + j] - base1
            picks[r, j] = jnp.clip(slot0, 0, pool - 1)
            picks[r, run_len + j] = jnp.clip(slot1, 0, pool - 1)
        picks[r, 2 * run_len] = run0 * (run_len * page_len)
        picks[r, 2 * run_len + 1] = run1 * (run_len * page_len)
        return carry

    lax.fori_loop(0, requests, find, 0)

    loads[0].wait()
    loads[1].wait()
    pl.semaphore_wait(barrier, seq_count)

    q_copies = {}
    for k in range(1, seq_count):
        peer = {"seq": flip(me, k, seq_count)}
        q_copies[k] = (
            pltpu.make_async_remote_copy(
                qlat.at[0], qlat.at[k], q_send_sem.at[0, k], q_recv_sem.at[0, k], device_id=peer
            ),
            pltpu.make_async_remote_copy(
                qrot.at[0], qrot.at[k], q_send_sem.at[1, k], q_recv_sem.at[1, k], device_id=peer
            ),
        )
        for copy in q_copies[k]:
            copy.start()
    other = {"head": 1 - core}
    page_copies = (
        pltpu.make_async_remote_copy(
            rot_hbm, rot_raw.at[1], page_send_sem.at[0], page_recv_sem.at[0], device_id=other
        ),
        pltpu.make_async_remote_copy(
            lat_hbm, cache.at[1], page_send_sem.at[1], page_recv_sem.at[1], device_id=other
        ),
    )
    for copy in page_copies:
        copy.start()

    lane_block = lax.broadcasted_iota(jnp.int32, (pool, LANES), 1) // rope

    def spread(half):
        for j in range(page_len // per_row):
            tile = rot_raw[half, :, j * LANES : (j + 1) * LANES].astype(jnp.float32)
            for b in range(per_row):
                rot_wide[pl.ds(j * per_row + b, pool, stride=page_len), :] = jnp.where(
                    lane_block == b, tile, 0.0
                )

        def narrow(p, carry):
            start = pl.multiple_of(p * page_len, page_len)
            rot_keys[half, p] = rot_wide[pl.ds(start, page_len), :].astype(jnp.bfloat16)
            return carry

        lax.fori_loop(0, pool, narrow, 0)

    loads[4].wait()
    spread(0)
    page_copies[0].wait_recv()
    spread(1)
    loads[5].wait()
    page_copies[1].wait_recv()

    row_block = lax.broadcasted_iota(jnp.int32, (heads // per_row, LANES), 1) // rope
    tokens = 2 * run_len * page_len
    token = lax.broadcasted_iota(jnp.int32, (1, tokens), 1)
    stat_lane = lax.broadcasted_iota(jnp.int32, (heads, LANES), 1)

    def partial(k):
        r = flip(me, k, seq_count)
        for i in range(heads // per_row):
            qrot_rows[i : i + 1, :] = qrot[k, :, i * LANES : (i + 1) * LANES].astype(jnp.float32)
        rows = qrot_rows[...]
        for b in range(per_row):
            only = jnp.where(row_block == b, rows, 0.0)
            full = only
            for turn in range(1, per_row):
                full = full + pltpu.roll(only, turn * rope, 1)
            qrot_wide[pl.ds(b, heads // per_row, stride=per_row), :] = full
        query_rot = qrot_wide[...].astype(jnp.bfloat16)
        where = [(h, picks[r, h * run_len + j]) for h in range(2) for j in range(run_len)]
        keys = jnp.concatenate([cache[h, p] for h, p in where], axis=0)
        rots = jnp.concatenate([rot_keys[h, p] for h, p in where], axis=0)
        contract = (((1,), (1,)), ((), ()))
        scores = lax.dot_general(qlat[k], keys, contract, preferred_element_type=jnp.float32)
        scores = scores + lax.dot_general(
            query_rot, rots, contract, preferred_element_type=jnp.float32
        )
        scores = scores * scale
        start = jnp.where(
            token < tokens // 2, picks[r, 2 * run_len], picks[r, 2 * run_len + 1] - tokens // 2
        )
        live = start + token < lens[r]
        scores = jnp.where(live, scores, MASKED_SCORE)
        top = jnp.max(scores, axis=1, keepdims=True)
        terms = jnp.where(live, jnp.exp(scores - top), 0.0)
        total = jnp.sum(terms, axis=1, keepdims=True)
        summed = jnp.dot(terms.astype(jnp.bfloat16), keys, preferred_element_type=jnp.float32)
        stats = jnp.where(stat_lane == 0, top, jnp.where(stat_lane == 1, total, 0.0))
        return summed, jnp.transpose(stats)[:8, :]

    p_copies = {}
    for k in range(1, seq_count):
        q_copies[k][0].wait_recv()
        q_copies[k][1].wait_recv()
        summed, stats = partial(k)
        part_send[k] = summed.astype(jnp.bfloat16)
        stat_send[k, :, :heads] = stats
        peer = {"seq": flip(me, k, seq_count)}
        p_copies[k] = (
            pltpu.make_async_remote_copy(
                stat_send.at[k],
                stat_recv.at[k],
                p_send_sem.at[0, k],
                p_recv_sem.at[0, k],
                device_id=peer,
            ),
            pltpu.make_async_remote_copy(
                part_send.at[k],
                part_recv.at[k],
                p_send_sem.at[1, k],
                p_recv_sem.at[1, k],
                device_id=peer,
            ),
        )
        for copy in p_copies[k]:
            copy.start()
    own, stats = partial(0)
    stat_recv[0, :, :heads] = stats

    for k in range(1, seq_count):
        p_copies[k][0].wait_recv()
    tops = [stat_recv[k, 0:1, :heads] for k in range(seq_count)]
    top = functools.reduce(jnp.maximum, tops)
    weights = [jnp.exp(t - top) for t in tops]
    total = sum(w * stat_recv[k, 1:2, :heads] for k, w in enumerate(weights))
    weights = [w / total for w in weights]
    pad = -seq_count % 8
    stacked = jnp.concatenate(weights + [jnp.zeros((pad, heads), jnp.float32)] * (pad > 0), axis=0)
    columns = jnp.transpose(stacked)
    result = own * columns[:, 0:1]
    for k in range(1, seq_count):
        p_copies[k][1].wait_recv()
        result = result + part_recv[k].astype(jnp.float32) * columns[:, k : k + 1]
    out_ref[0] = result.astype(jnp.bfloat16)

    for k in range(1, seq_count):
        for copy in q_copies[k] + p_copies[k]:
            copy.wait_send()
    for copy in page_copies:
        copy.wait_send()


def local(q_latent, q_rope, cache_latent, cache_rope, page_table, lengths):
    seq_count = lax.axis_size("seq")
    head_count = lax.axis_size("head")
    pool, page_len, latent = cache_latent.shape
    heads = q_latent.shape[1]
    requests, slots = page_table.shape
    run_len = slots // (seq_count * head_count)
    anywhere = pl.BlockSpec(memory_space=pl.ANY)
    bf16, f32, i32 = jnp.bfloat16, jnp.float32, jnp.int32
    dma = pltpu.SemaphoreType.DMA
    return pl.pallas_call(
        functools.partial(kernel, seq_count, run_len),
        out_shape=jax.ShapeDtypeStruct(q_latent.shape, bf16),
        in_specs=[anywhere] * 6,
        out_specs=pl.BlockSpec(memory_space=pltpu.VMEM),
        scratch_shapes=[
            pltpu.VMEM((2, pool, page_len, latent), bf16),
            pltpu.VMEM((2,) + cache_rope.shape, bf16),
            pltpu.VMEM((pool * page_len, LANES), f32),
            pltpu.VMEM((2, pool, page_len, LANES), bf16),
            pltpu.VMEM((seq_count, heads, latent), bf16),
            pltpu.VMEM((seq_count, 1, q_rope.shape[1]), bf16),
            pltpu.VMEM((heads * cache_rope.shape[1] // page_len // LANES, LANES), f32),
            pltpu.VMEM((heads, LANES), f32),
            pltpu.VMEM((seq_count, heads, latent), bf16),
            pltpu.VMEM((seq_count, heads, latent), bf16),
            pltpu.VMEM((seq_count, 8, LANES), f32),
            pltpu.VMEM((seq_count, 8, LANES), f32),
            pltpu.SMEM((requests, slots), i32),
            pltpu.SMEM((requests,), i32),
            pltpu.SMEM((requests, 2 * run_len + 2), i32),
            dma((6,)),
            dma((2,)),
            dma((2,)),
            dma((2, seq_count)),
            dma((2, seq_count)),
            dma((2, seq_count)),
            dma((2, seq_count)),
        ],
        compiler_params=pltpu.CompilerParams(
            collective_id=0, has_side_effects=True, vmem_limit_bytes=60 * 2**20
        ),
    )(q_latent, q_rope, cache_latent, cache_rope, page_table, lengths)


def solution(mesh):
    return jax.shard_map(
        local,
        mesh=mesh,
        in_specs=(
            P(("groups", "seq"), "head", None),
            P(("groups", "seq"), "head"),
            P(("groups", "seq", "head"), None, None),
            P(("groups", "seq", "head"), None),
            P("groups", None),
            P("groups"),
        ),
        out_specs=P(("groups", "seq"), "head", None),
        check_vma=False,
    )
```

```python
import functools
import math

import jax
import jax.numpy as jnp
from jax import lax
from jax.experimental import pallas as pl
from jax.experimental.pallas import tpu as pltpu
from jax.sharding import PartitionSpec as P

ROPE = 64
NOPE = 128
LANES = 128
MASKED_SCORE = -1e30
PAIR = 2


def kernel(
    seq_count,
    run_len,
    qlat_hbm,
    qrot_hbm,
    lat_hbm,
    rot_hbm,
    table_hbm,
    len_hbm,
    out_ref,
    cache,
    rot_raw,
    rot_wide,
    rot_keys,
    qlat,
    qrot,
    qrot_rows,
    qrot_wide,
    part_send,
    part_recv,
    stat_send,
    stat_recv,
    table,
    lens,
    picks,
    local_sem,
    page_send_sem,
    page_recv_sem,
    q_send_sem,
    q_recv_sem,
    p_send_sem,
    p_recv_sem,
):
    me = lax.axis_index("seq")
    core = lax.axis_index("head")
    pool, page_len, latent = lat_hbm.shape
    heads = qlat.shape[1]
    rope = qrot.shape[2] // heads
    per_row = LANES // rope
    requests, slots = table.shape
    runs = slots // run_len
    scale = 1.0 / math.sqrt(NOPE + ROPE)

    loads = [
        pltpu.make_async_copy(qlat_hbm, qlat.at[pl.ds(0, 1)], local_sem.at[0]),
        pltpu.make_async_copy(qrot_hbm, qrot.at[0], local_sem.at[1]),
        pltpu.make_async_copy(table_hbm, table, local_sem.at[2]),
        pltpu.make_async_copy(len_hbm, lens, local_sem.at[3]),
        pltpu.make_async_copy(rot_hbm, rot_raw.at[0], local_sem.at[4]),
        pltpu.make_async_copy(lat_hbm, cache.at[0], local_sem.at[5]),
    ]
    for load in loads:
        load.start()

    ring = seq_count // PAIR
    half_way = ring // 2
    row, column = me // PAIR, me % PAIR

    def slot(step, cross):
        return (step % ring) * PAIR + cross

    def index_of(step, cross):
        col = 1 - column if cross else column
        return ((row + step % ring) % ring) * PAIR + col

    right, left, across = index_of(1, 0), index_of(-1, 0), index_of(0, 1)
    barrier = pltpu.get_barrier_semaphore()
    for peer in (right, left, across):
        pl.semaphore_signal(barrier, inc=1, device_id={"seq": peer})
    pl.semaphore_signal(barrier, inc=1, device_id={"head": 1 - core})
    loads[0].wait()
    loads[1].wait()
    pl.semaphore_wait(barrier, 4)

    sent = []
    arrivals = {}
    first_rows, last_rows = pl.ds(0, heads // 2), pl.ds(heads // 2, heads // 2)

    def push(ref, piece, source, target, peer, rows=None):
        here, there = ref.at[source], ref.at[target]
        if rows is not None:
            here, there = ref.at[source, rows], ref.at[target, rows]
        copy = pltpu.make_async_remote_copy(
            here,
            there,
            q_send_sem.at[len(sent)],
            q_recv_sem.at[piece, target],
            device_id={"seq": peer},
        )
        copy.start()
        sent.append(copy)
        arrivals.setdefault(target, []).append(copy)

    def push_all(source, target, peer):
        push(qlat, 0, source, target, peer)
        push(qrot, 1, source, target, peer)

    def arrive(target, which=slice(None)):
        for copy in arrivals[target][which]:
            copy.wait_recv()

    push_all(0, slot(-1, 0), right)
    push_all(0, slot(1, 0), left)
    push_all(0, slot(0, 1), across)
    other = {"head": 1 - core}
    page_copies = (
        pltpu.make_async_remote_copy(
            rot_hbm, rot_raw.at[1], page_send_sem.at[0], page_recv_sem.at[0], device_id=other
        ),
        pltpu.make_async_remote_copy(
            lat_hbm, cache.at[1], page_send_sem.at[1], page_recv_sem.at[1], device_id=other
        ),
    )
    for copy in page_copies:
        copy.start()

    loads[2].wait()
    loads[3].wait()
    base0 = (me * 2 + core) * pool
    base1 = (me * 2 + 1 - core) * pool

    chunk = math.gcd(runs, 16)

    def find(r, carry):
        def scan(c, found):
            run0, run1 = found
            for i in range(chunk):
                run = c * chunk + i
                first = table[r, run * run_len]
                run0 = jnp.where((first >= base0) & (first < base0 + pool), run, run0)
                run1 = jnp.where((first >= base1) & (first < base1 + pool), run, run1)
            return run0, run1

        zero = jnp.int32(0)
        if runs == chunk:
            run0, run1 = scan(0, (zero, zero))
        else:
            run0, run1 = lax.fori_loop(0, runs // chunk, scan, (zero, zero))
        for j in range(run_len):
            slot0 = table[r, run0 * run_len + j] - base0
            slot1 = table[r, run1 * run_len + j] - base1
            picks[r, j] = jnp.clip(slot0, 0, pool - 1)
            picks[r, run_len + j] = jnp.clip(slot1, 0, pool - 1)
        picks[r, 2 * run_len] = run0 * (run_len * page_len)
        picks[r, 2 * run_len + 1] = run1 * (run_len * page_len)
        return carry

    lax.fori_loop(0, requests, find, 0)

    lane_block = lax.broadcasted_iota(jnp.int32, (pool, LANES), 1) // rope

    def spread(half):
        for j in range(page_len // per_row):
            tile = rot_raw[half, :, j * LANES : (j + 1) * LANES].astype(jnp.float32)
            for b in range(per_row):
                rot_wide[pl.ds(j * per_row + b, pool, stride=page_len), :] = jnp.where(
                    lane_block == b, tile, 0.0
                )

        def narrow(p, carry):
            start = pl.multiple_of(p * page_len, page_len)
            rot_keys[half, p] = rot_wide[pl.ds(start, page_len), :].astype(jnp.bfloat16)
            return carry

        lax.fori_loop(0, pool, narrow, 0)

    loads[4].wait()
    spread(0)

    def turn_back(step):
        arrive(slot(step, 0))
        push(qlat, 0, slot(step, 0), slot(half_way, 0), left, first_rows)
        push(qrot, 1, slot(step, 0), slot(half_way, 0), left)
        arrive(slot(-step, 0))
        push(qlat, 2, slot(-step, 0), slot(half_way, 0), right, last_rows)

    for step in range(1, half_way):
        if step == half_way - 1:
            turn_back(step)
        else:
            arrive(slot(step, 0))
            push_all(slot(step, 0), slot(step + 1, 0), left)
            arrive(slot(-step, 0))
            push_all(slot(-step, 0), slot(-step - 1, 0), right)
        arrive(slot(step - 1, 1))
        push_all(slot(step - 1, 1), slot(step, 1), left)
        if step > 1:
            arrive(slot(1 - step, 1))
        push_all(slot(1 - step, 1), slot(-step, 1), right)
    page_copies[0].wait_recv()
    spread(1)
    arrive(slot(half_way, 0), slice(0, 2))
    push(qlat, 0, slot(half_way, 0), slot(half_way, 1), across, first_rows)
    push(qrot, 1, slot(half_way, 0), slot(half_way, 1), across)
    arrive(slot(half_way, 0), slice(2, 3))
    push(qlat, 2, slot(half_way, 0), slot(half_way, 1), across, last_rows)
    loads[5].wait()
    page_copies[1].wait_recv()

    row_block = lax.broadcasted_iota(jnp.int32, (heads // per_row, LANES), 1) // rope
    tokens = 2 * run_len * page_len
    token = lax.broadcasted_iota(jnp.int32, (1, tokens), 1)
    stat_lane = lax.broadcasted_iota(jnp.int32, (heads, LANES), 1)

    def partial(k, r):
        for i in range(heads // per_row):
            qrot_rows[i : i + 1, :] = qrot[k, :, i * LANES : (i + 1) * LANES].astype(jnp.float32)
        rows = qrot_rows[...]
        for b in range(per_row):
            only = jnp.where(row_block == b, rows, 0.0)
            full = only
            for turn in range(1, per_row):
                full = full + pltpu.roll(only, turn * rope, 1)
            qrot_wide[pl.ds(b, heads // per_row, stride=per_row), :] = full
        query_rot = qrot_wide[...].astype(jnp.bfloat16)
        where = [(h, picks[r, h * run_len + j]) for h in range(2) for j in range(run_len)]
        keys = jnp.concatenate([cache[h, p] for h, p in where], axis=0)
        rots = jnp.concatenate([rot_keys[h, p] for h, p in where], axis=0)
        contract = (((1,), (1,)), ((), ()))
        scores = lax.dot_general(qlat[k], keys, contract, preferred_element_type=jnp.float32)
        scores = scores + lax.dot_general(
            query_rot, rots, contract, preferred_element_type=jnp.float32
        )
        scores = scores * scale
        start = jnp.where(
            token < tokens // 2, picks[r, 2 * run_len], picks[r, 2 * run_len + 1] - tokens // 2
        )
        live = start + token < lens[r]
        scores = jnp.where(live, scores, MASKED_SCORE)
        top = jnp.max(scores, axis=1, keepdims=True)
        terms = jnp.where(live, jnp.exp(scores - top), 0.0)
        total = jnp.sum(terms, axis=1, keepdims=True)
        summed = jnp.dot(terms.astype(jnp.bfloat16), keys, preferred_element_type=jnp.float32)
        stats = jnp.where(stat_lane == 0, top, jnp.where(stat_lane == 1, total, 0.0))
        return summed, jnp.transpose(stats)[:8, :]

    order = [(0, 1)]
    for step in range(1, half_way):
        order += [(step, 0), (-step, 0)]
    late = [(step * sign, 1) for step in range(1, half_way) for sign in (1, -1)]
    order += [(0, 0)] + late + [(half_way, 0), (half_way, 1)]
    relayed = {slot(step, 1) for step in range(half_way - 1)}
    relayed |= {slot(-step, 1) for step in range(half_way - 1)}
    p_copies = {}
    for step, cross in order:
        k, r = slot(step, cross), index_of(step, cross)
        if k == 0:
            own, stats = partial(0, me)
            stat_recv[0, :, :heads] = stats
            continue
        if cross and k not in relayed:
            arrive(k)
        summed, stats = partial(k, r)
        part_send[k] = summed.astype(jnp.bfloat16)
        stat_send[k, :, :heads] = stats
        back = slot(-step, cross)
        p_copies[k] = (
            pltpu.make_async_remote_copy(
                stat_send.at[k],
                stat_recv.at[back],
                p_send_sem.at[0, k],
                p_recv_sem.at[0, back],
                device_id={"seq": r},
            ),
            pltpu.make_async_remote_copy(
                part_send.at[k],
                part_recv.at[back],
                p_send_sem.at[1, k],
                p_recv_sem.at[1, back],
                device_id={"seq": r},
            ),
        )
        for copy in p_copies[k]:
            copy.start()

    for k in range(1, seq_count):
        p_copies[k][0].wait_recv()
    tops = [stat_recv[k, 0:1, :heads] for k in range(seq_count)]
    top = functools.reduce(jnp.maximum, tops)
    weights = [jnp.exp(t - top) for t in tops]
    total = sum(w * stat_recv[k, 1:2, :heads] for k, w in enumerate(weights))
    weights = [w / total for w in weights]
    pad = -seq_count % 8
    stacked = jnp.concatenate(weights + [jnp.zeros((pad, heads), jnp.float32)] * (pad > 0), axis=0)
    columns = jnp.transpose(stacked)
    result = own * columns[:, 0:1]
    for step, cross in order:
        k, back = slot(step, cross), slot(-step, cross)
        if k > 0:
            p_copies[k][1].wait_recv()
            result = result + part_recv[back].astype(jnp.float32) * columns[:, back : back + 1]
    out_ref[0] = result.astype(jnp.bfloat16)

    for k in range(1, seq_count):
        for copy in p_copies[k]:
            copy.wait_send()
    for copy in sent + list(page_copies):
        copy.wait_send()


def local(q_latent, q_rope, cache_latent, cache_rope, page_table, lengths):
    seq_count = lax.axis_size("seq")
    head_count = lax.axis_size("head")
    pool, page_len, latent = cache_latent.shape
    heads = q_latent.shape[1]
    requests, slots = page_table.shape
    run_len = slots // (seq_count * head_count)
    anywhere = pl.BlockSpec(memory_space=pl.ANY)
    bf16, f32, i32 = jnp.bfloat16, jnp.float32, jnp.int32
    dma = pltpu.SemaphoreType.DMA
    return pl.pallas_call(
        functools.partial(kernel, seq_count, run_len),
        out_shape=jax.ShapeDtypeStruct(q_latent.shape, bf16),
        in_specs=[anywhere] * 6,
        out_specs=pl.BlockSpec(memory_space=pltpu.VMEM),
        scratch_shapes=[
            pltpu.VMEM((2, pool, page_len, latent), bf16),
            pltpu.VMEM((2,) + cache_rope.shape, bf16),
            pltpu.VMEM((pool * page_len, LANES), f32),
            pltpu.VMEM((2, pool, page_len, LANES), bf16),
            pltpu.VMEM((seq_count, heads, latent), bf16),
            pltpu.VMEM((seq_count, 1, q_rope.shape[1]), bf16),
            pltpu.VMEM((heads * cache_rope.shape[1] // page_len // LANES, LANES), f32),
            pltpu.VMEM((heads, LANES), f32),
            pltpu.VMEM((seq_count, heads, latent), bf16),
            pltpu.VMEM((seq_count, heads, latent), bf16),
            pltpu.VMEM((seq_count, 8, LANES), f32),
            pltpu.VMEM((seq_count, 8, LANES), f32),
            pltpu.SMEM((requests, slots), i32),
            pltpu.SMEM((requests,), i32),
            pltpu.SMEM((requests, 2 * run_len + 2), i32),
            dma((6,)),
            dma((2,)),
            dma((2,)),
            dma((3 * seq_count,)),
            dma((3, seq_count)),
            dma((2, seq_count)),
            dma((2, seq_count)),
        ],
        compiler_params=pltpu.CompilerParams(
            collective_id=0, has_side_effects=True, vmem_limit_bytes=60 * 2**20
        ),
    )(q_latent, q_rope, cache_latent, cache_rope, page_table, lengths)


def solution(mesh):
    return jax.shard_map(
        local,
        mesh=mesh,
        in_specs=(
            P(("groups", "seq"), "head", None),
            P(("groups", "seq"), "head"),
            P(("groups", "seq", "head"), None, None),
            P(("groups", "seq", "head"), None),
            P("groups", None),
            P("groups"),
        ),
        out_specs=P(("groups", "seq"), "head", None),
        check_vma=False,
    )
```

```python
import functools
import math

import jax
import jax.numpy as jnp
from jax import lax
from jax.experimental import pallas as pl
from jax.experimental.pallas import tpu as pltpu
from jax.sharding import PartitionSpec as P

ROPE = 64
NOPE = 128
LANES = 128
MASKED_SCORE = -1e30


def flip(index, mask, count):
    result = index
    bit = 1
    while bit < count:
        if mask & bit:
            result = result + bit * (1 - 2 * ((index // bit) % 2))
        bit *= 2
    return result


def kernel(
    seq_count,
    run_len,
    qlat_hbm,
    qrot_hbm,
    lat_hbm,
    rot_hbm,
    table_hbm,
    len_hbm,
    out_ref,
    cache,
    rot_raw,
    rot_wide,
    rot_keys,
    qlat,
    qrot,
    qrot_rows,
    qrot_wide,
    part_send,
    part_recv,
    stat_send,
    stat_recv,
    table,
    lens,
    picks,
    local_sem,
    page_send_sem,
    page_recv_sem,
    q_send_sem,
    q_recv_sem,
    p_send_sem,
    p_recv_sem,
):
    me = lax.axis_index("seq")
    core = lax.axis_index("head")
    pool, page_len, latent = lat_hbm.shape
    heads = qlat.shape[1]
    rope = qrot.shape[2] // heads
    per_row = LANES // rope
    requests, slots = table.shape
    runs = slots // run_len
    scale = 1.0 / math.sqrt(NOPE + ROPE)

    loads = [
        pltpu.make_async_copy(qlat_hbm, qlat.at[pl.ds(0, 1)], local_sem.at[0]),
        pltpu.make_async_copy(qrot_hbm, qrot.at[0], local_sem.at[1]),
        pltpu.make_async_copy(table_hbm, table, local_sem.at[2]),
        pltpu.make_async_copy(len_hbm, lens, local_sem.at[3]),
        pltpu.make_async_copy(rot_hbm, rot_raw.at[0], local_sem.at[4]),
        pltpu.make_async_copy(lat_hbm, cache.at[0], local_sem.at[5]),
    ]
    for load in loads:
        load.start()

    barrier = pltpu.get_barrier_semaphore()
    for k in range(1, seq_count):
        pl.semaphore_signal(barrier, inc=1, device_id={"seq": flip(me, k, seq_count)})
    pl.semaphore_signal(barrier, inc=1, device_id={"head": 1 - core})

    loads[2].wait()
    loads[3].wait()
    base0 = (me * 2 + core) * pool
    base1 = (me * 2 + 1 - core) * pool

    chunk = math.gcd(runs, 16)

    def find(r, carry):
        def scan(c, found):
            run0, run1 = found
            for i in range(chunk):
                run = c * chunk + i
                first = table[r, run * run_len]
                run0 = jnp.where((first >= base0) & (first < base0 + pool), run, run0)
                run1 = jnp.where((first >= base1) & (first < base1 + pool), run, run1)
            return run0, run1

        zero = jnp.int32(0)
        if runs == chunk:
            run0, run1 = scan(0, (zero, zero))
        else:
            run0, run1 = lax.fori_loop(0, runs // chunk, scan, (zero, zero))
        for j in range(run_len):
            slot0 = table[r, run0 * run_len + j] - base0
            slot1 = table[r, run1 * run_len + j] - base1
            picks[r, j] = jnp.clip(slot0, 0, pool - 1)
            picks[r, run_len + j] = jnp.clip(slot1, 0, pool - 1)
        picks[r, 2 * run_len] = run0 * (run_len * page_len)
        picks[r, 2 * run_len + 1] = run1 * (run_len * page_len)
        return carry

    lax.fori_loop(0, requests, find, 0)

    loads[0].wait()
    loads[1].wait()
    pl.semaphore_wait(barrier, seq_count)

    half_way, relayed = seq_count // 2, seq_count // 2 + 1
    same = [k for k in range(2, seq_count, 2) if k != half_way]
    cross = [k for k in range(3, seq_count, 2) if k != relayed]
    sends = [half_way] + same + cross + [1]

    def query_copies(source, target, peer):
        copies = [
            pltpu.make_async_remote_copy(
                ref.at[source],
                ref.at[target],
                q_send_sem.at[part, target],
                q_recv_sem.at[part, target],
                device_id={"seq": flip(me, peer, seq_count)},
            )
            for part, ref in enumerate((qlat, qrot))
        ]
        for copy in copies:
            copy.start()
        return tuple(copies)

    q_copies = {k: query_copies(0, k, k) for k in sends}
    other = {"head": 1 - core}
    page_copies = (
        pltpu.make_async_remote_copy(
            rot_hbm, rot_raw.at[1], page_send_sem.at[0], page_recv_sem.at[0], device_id=other
        ),
        pltpu.make_async_remote_copy(
            lat_hbm, cache.at[1], page_send_sem.at[1], page_recv_sem.at[1], device_id=other
        ),
    )
    for copy in page_copies:
        copy.start()

    lane_block = lax.broadcasted_iota(jnp.int32, (pool, LANES), 1) // rope

    def spread(half):
        for j in range(page_len // per_row):
            tile = rot_raw[half, :, j * LANES : (j + 1) * LANES].astype(jnp.float32)
            for b in range(per_row):
                rot_wide[pl.ds(j * per_row + b, pool, stride=page_len), :] = jnp.where(
                    lane_block == b, tile, 0.0
                )

        def narrow(p, carry):
            start = pl.multiple_of(p * page_len, page_len)
            rot_keys[half, p] = rot_wide[pl.ds(start, page_len), :].astype(jnp.bfloat16)
            return carry

        lax.fori_loop(0, pool, narrow, 0)

    loads[4].wait()
    spread(0)
    for copy in q_copies[half_way]:
        copy.wait_recv()
    q_copies[relayed] = query_copies(half_way, relayed, 1)
    page_copies[0].wait_recv()
    spread(1)
    loads[5].wait()
    page_copies[1].wait_recv()

    row_block = lax.broadcasted_iota(jnp.int32, (heads // per_row, LANES), 1) // rope
    tokens = 2 * run_len * page_len
    token = lax.broadcasted_iota(jnp.int32, (1, tokens), 1)
    stat_lane = lax.broadcasted_iota(jnp.int32, (heads, LANES), 1)

    def partial(k):
        r = flip(me, k, seq_count)
        for i in range(heads // per_row):
            qrot_rows[i : i + 1, :] = qrot[k, :, i * LANES : (i + 1) * LANES].astype(jnp.float32)
        rows = qrot_rows[...]
        for b in range(per_row):
            only = jnp.where(row_block == b, rows, 0.0)
            full = only
            for turn in range(1, per_row):
                full = full + pltpu.roll(only, turn * rope, 1)
            qrot_wide[pl.ds(b, heads // per_row, stride=per_row), :] = full
        query_rot = qrot_wide[...].astype(jnp.bfloat16)
        where = [(h, picks[r, h * run_len + j]) for h in range(2) for j in range(run_len)]
        keys = jnp.concatenate([cache[h, p] for h, p in where], axis=0)
        rots = jnp.concatenate([rot_keys[h, p] for h, p in where], axis=0)
        contract = (((1,), (1,)), ((), ()))
        scores = lax.dot_general(qlat[k], keys, contract, preferred_element_type=jnp.float32)
        scores = scores + lax.dot_general(
            query_rot, rots, contract, preferred_element_type=jnp.float32
        )
        scores = scores * scale
        start = jnp.where(
            token < tokens // 2, picks[r, 2 * run_len], picks[r, 2 * run_len + 1] - tokens // 2
        )
        live = start + token < lens[r]
        scores = jnp.where(live, scores, MASKED_SCORE)
        top = jnp.max(scores, axis=1, keepdims=True)
        terms = jnp.where(live, jnp.exp(scores - top), 0.0)
        total = jnp.sum(terms, axis=1, keepdims=True)
        summed = jnp.dot(terms.astype(jnp.bfloat16), keys, preferred_element_type=jnp.float32)
        stats = jnp.where(stat_lane == 0, top, jnp.where(stat_lane == 1, total, 0.0))
        return summed, jnp.transpose(stats)[:2, :]

    p_copies = {}
    order = sends + [relayed]
    for k in order:
        if k != half_way:
            for copy in q_copies[k]:
                copy.wait_recv()
        summed, stats = partial(k)
        part_send[k] = summed.astype(jnp.bfloat16)
        stat_send[k, :, :heads] = stats
        peer = {"seq": flip(me, k, seq_count)}
        p_copies[k] = (
            pltpu.make_async_remote_copy(
                stat_send.at[k],
                stat_recv.at[k],
                p_send_sem.at[0, k],
                p_recv_sem.at[0, k],
                device_id=peer,
            ),
            pltpu.make_async_remote_copy(
                part_send.at[k],
                part_recv.at[k],
                p_send_sem.at[1, k],
                p_recv_sem.at[1, k],
                device_id=peer,
            ),
        )
        for copy in p_copies[k]:
            copy.start()
    own, stats = partial(0)
    stat_recv[0, :, :heads] = stats

    for k in range(1, seq_count):
        p_copies[k][0].wait_recv()
    tops = [stat_recv[k, 0:1, :heads] for k in range(seq_count)]
    top = functools.reduce(jnp.maximum, tops)
    weights = [jnp.exp(t - top) for t in tops]
    total = sum(w * stat_recv[k, 1:2, :heads] for k, w in enumerate(weights))
    weights = [w / total for w in weights]
    pad = -seq_count % 8
    stacked = jnp.concatenate(weights + [jnp.zeros((pad, heads), jnp.float32)] * (pad > 0), axis=0)
    columns = jnp.transpose(stacked)
    result = own * columns[:, 0:1]
    for k in order:
        p_copies[k][1].wait_recv()
        result = result + part_recv[k].astype(jnp.float32) * columns[:, k : k + 1]
    out_ref[0] = result.astype(jnp.bfloat16)

    for k in range(1, seq_count):
        for copy in q_copies[k] + p_copies[k]:
            copy.wait_send()
    for copy in page_copies:
        copy.wait_send()


def local(q_latent, q_rope, cache_latent, cache_rope, page_table, lengths):
    seq_count = lax.axis_size("seq")
    head_count = lax.axis_size("head")
    pool, page_len, latent = cache_latent.shape
    heads = q_latent.shape[1]
    requests, slots = page_table.shape
    run_len = slots // (seq_count * head_count)
    anywhere = pl.BlockSpec(memory_space=pl.ANY)
    bf16, f32, i32 = jnp.bfloat16, jnp.float32, jnp.int32
    dma = pltpu.SemaphoreType.DMA
    return pl.pallas_call(
        functools.partial(kernel, seq_count, run_len),
        out_shape=jax.ShapeDtypeStruct(q_latent.shape, bf16),
        in_specs=[anywhere] * 6,
        out_specs=pl.BlockSpec(memory_space=pltpu.VMEM),
        scratch_shapes=[
            pltpu.VMEM((2, pool, page_len, latent), bf16),
            pltpu.VMEM((2,) + cache_rope.shape, bf16),
            pltpu.VMEM((pool * page_len, LANES), f32),
            pltpu.VMEM((2, pool, page_len, LANES), bf16),
            pltpu.VMEM((seq_count, heads, latent), bf16),
            pltpu.VMEM((seq_count, 1, q_rope.shape[1]), bf16),
            pltpu.VMEM((heads * cache_rope.shape[1] // page_len // LANES, LANES), f32),
            pltpu.VMEM((heads, LANES), f32),
            pltpu.VMEM((seq_count, heads, latent), bf16),
            pltpu.VMEM((seq_count, heads, latent), bf16),
            pltpu.VMEM((seq_count, 2, LANES), f32),
            pltpu.VMEM((seq_count, 2, LANES), f32),
            pltpu.SMEM((requests, slots), i32),
            pltpu.SMEM((requests,), i32),
            pltpu.SMEM((requests, 2 * run_len + 2), i32),
            dma((6,)),
            dma((2,)),
            dma((2,)),
            dma((2, seq_count)),
            dma((2, seq_count)),
            dma((2, seq_count)),
            dma((2, seq_count)),
        ],
        compiler_params=pltpu.CompilerParams(
            collective_id=0, has_side_effects=True, vmem_limit_bytes=60 * 2**20
        ),
    )(q_latent, q_rope, cache_latent, cache_rope, page_table, lengths)


def solution(mesh):
    return jax.shard_map(
        local,
        mesh=mesh,
        in_specs=(
            P(("groups", "seq"), "head", None),
            P(("groups", "seq"), "head"),
            P(("groups", "seq", "head"), None, None),
            P(("groups", "seq", "head"), None),
            P("groups", None),
            P("groups"),
        ),
        out_specs=P(("groups", "seq"), "head", None),
        check_vma=False,
    )
```
